256 devices in a mesh: seq: 32 (over x, z), head: 8 (over y, core).
Axes of the slice: x: 4, y: 4, z: 8, core: 2. Of those that a mesh axis runs over, the one named last changes fastest.
Arguments:
- inner_input: bfloat16 [16384, 16384], P('seq', 'head'), may hold values from -6 to 6
- state_input: bfloat16 [16384, 4096], P('seq', 'head'), may hold values from -6 to 6
- gate_input: bfloat16 [16384, 16384], P('seq', 'head'), may hold values from -6 to 6
- inner_taps: bfloat16 [4, 16384], P(None, 'head'), may hold values from -3 to 3
- inner_bias: bfloat16 [16384], P('head'), may hold values from -3 to 3
- state_taps: bfloat16 [4, 4096], P(None, 'head'), may hold values from -3 to 3
- state_bias: bfloat16 [4096], P('head'), may hold values from -3 to 3
- step_raw: float32 [256, 16384], P('head', 'seq'), may hold values from -5.3 to -1
- step_bias: float32 [256], P('head'), may hold values from -0.5 to 0.5
- decay_log: float32 [256], P('head'), may hold values from -9 to 1.26
- skip_gain: float32 [256], P('head'), may hold values from 0.5 to 1.5
- norm_gain: bfloat16 [16384], P('head'), may hold values from 0.5 to 1.5
- out_weight: bfloat16 [16384, 4096], P('head', 'seq'), may hold values from -0.09375 to 0.09375
- sequence_lengths: int32 [4], replicated, may hold values from 1 to 8192, 16384 in all
Outputs:
- mixed_out: bfloat16 [16384, 4096], P('seq', 'head')
The draws below stay inside these ranges and needn't reach their ends.
Inputs may be any that keep to these rules, and one draw needn't show every extreme that they name: `sequence_lengths`: the 4 sequences lie end to end in the order given and fill all 16384 positions; the longest has exactly 8192 positions.
All inputs are finite; a program needn't handle non-finite values.
Results may differ from the reference program's by a relative error of at most 0.018.
Values may be sent and summed in bfloat16 or wider, within the bound.
No kernel may reach another device: no remote copies, remote signals or barrier semaphores. Data moves between devices by JAX's collectives and lax.ppermute only.
A program may use at most 256 MiB of HBM per device.

```python
import math
from functools import partial
import jax
import jax.numpy as jnp
import numpy as np
from jax import lax

HEAD_COUNT = 256
HEAD_DIM = 64
STATE_DIM = 256
GROUP_COUNT = 8
CONV_WIDTH = 4
BLOCK_LEN = 256
OUT_WIDTH = 4096
SEQ_COUNT = 4
INNER_DIM = 16384
PACKED_TOKENS = 16384
N_HEAD = 8


def draw_step_raw(key, part):
    level_key = jax.random.fold_in(key, 11)
    cluster_random_key = jax.random.fold_in(key, 12)
    noise_levels = jax.random.uniform(level_key, (HEAD_COUNT, PACKED_TOKENS), jnp.float32, -5.3, -3.9)
    sample_locations = jax.random.randint(cluster_random_key, (4,), 0, PACKED_TOKENS)
    token_locations = lax.iota(jnp.int32, PACKED_TOKENS)
    token_clusters = jnp.any(token_locations[None, :] == sample_locations[:, None], axis=0)
    return jnp.where(token_clusters[None, :], -1.0, noise_levels).astype(jnp.float32)


def draw_decay_log(key, part):
    pick_key = jax.random.fold_in(key, 21)
    slow_key = jax.random.fold_in(key, 22)
    fast_key = jax.random.fold_in(key, 23)
    share = 0.5
    slow_pick = jax.random.uniform(pick_key, (HEAD_COUNT,), jnp.float32) < share
    slow_value = jnp.log(20.0 / PACKED_TOKENS) + jnp.log(10.0) * jax.random.uniform(slow_key, (HEAD_COUNT,), jnp.float32)
    fast_value = jnp.log(jax.random.uniform(fast_key, (HEAD_COUNT,), jnp.float32, 2.0, 3.5))
    return jnp.where(slow_pick, slow_value, fast_value).astype(jnp.float32)


def raised(values, rng, source, target, parts, factor):
    def block_of(axis_at):
        return (jnp.arange(values.shape[axis_at]) // (values.shape[axis_at] // parts)).reshape((-1,) + (1,) * (values.ndim - 1 - axis_at))

    near = jax.random.permutation(rng, parts)[block_of(target)]
    second = (block_of(target) + parts // 2) % parts
    return jnp.where((block_of(source) == near) | (block_of(source) == second), factor * values, values)


def level_of(own_key, dims, shards, smallest, high):
    loudness, own = 1.0, jax.random.fold_in(own_key, 6)
    for dim, parts in shards:
        steps = jnp.exp(jax.random.uniform(jax.random.fold_in(own, dim), (parts,), jnp.float32, smallest / len(shards), high / len(shards)))
        loudness = loudness * jnp.repeat(steps, dims[dim] // parts).reshape([-1 if axis == dim else 1 for axis in range(len(dims))])
    return loudness


def length_profile(count, total, most, skew):
    portions = [(1 << 20) // math.isqrt(grade ** skew) + 1 for grade in range(2, count + 1)]
    rest, holding = total - most - (count - 1), [1] * (count - 1)
    while rest > 0:
        movable = [i for i in range(count - 1) if holding[i] < most]
        mass, left = sum([portions[i] for i in movable]), rest
        for i in movable:
            more = min(most - holding[i], max(1, left * portions[i] // mass), rest)
            holding[i] = holding[i] + more
            rest = rest - more
    return np.array([most] + holding)


def uneven(rng, number_of, total, most, skew):
    if number_of == 2:
        one = jax.random.randint(rng, (), max(1, total - most), min(most, total - 1) + 1)
        return jnp.stack([one, total - one])
    lengths = jnp.asarray(length_profile(number_of, total, most, skew), jnp.int32)
    twos = (number_of - 1) // 2
    donor, taker = lengths[1:1 + 2 * twos:2], lengths[2:2 + 2 * twos:2]
    room = jnp.minimum(donor - 1, most - taker)
    passed = jax.random.randint(jax.random.fold_in(rng, 1), (twos,), 0, 1 << 20) % (room + 1)
    lengths = lengths.at[1:1 + 2 * twos:2].set(donor - passed).at[2:2 + 2 * twos:2].set(taker + passed)
    return lengths[jax.random.permutation(jax.random.fold_in(rng, 2), number_of)]


def bell_draw(stream_key, dims, scale, bound, shards=(), held_as=jnp.bfloat16):
    drawn = scale * jax.random.normal(stream_key, dims, jnp.float32)
    if shards:
        drawn = drawn * level_of(stream_key, dims, shards, -0.22, 0.18)
    return jnp.clip(drawn, -bound, bound).astype(held_as)


def noise_with(own_key, extent, deviation, limit, pieces, heavy, held_as=jnp.bfloat16):
    array = deviation * jax.random.normal(own_key, extent, jnp.float32)
    if pieces:
        array = array * level_of(own_key, extent, pieces, -0.22, 0.18)
    return jnp.clip(raised(array, jax.random.fold_in(own_key, 3), *heavy), -limit, limit).astype(held_as)


def setup_inputs(seed: int = 0) -> dict:
    splits = jax.random.split(jax.random.key(seed), 15)
    return {
        "inner_input": bell_draw(splits[0], (PACKED_TOKENS, INNER_DIM), 1.0, 6.0, ((0, 32), (1, 8))),
        "state_input": bell_draw(splits[1], (PACKED_TOKENS, GROUP_COUNT * 2 * STATE_DIM), 1.0, 6.0, ((0, 32), (1, 8))),
        "gate_input": bell_draw(splits[2], (PACKED_TOKENS, INNER_DIM), 1.0, 6.0, ((0, 32), (1, 8))),
        "inner_taps": bell_draw(splits[3], (CONV_WIDTH, INNER_DIM), CONV_WIDTH ** -0.5, 3.0, ((1, 8),)),
        "inner_bias": bell_draw(splits[4], (INNER_DIM,), 0.5, 3.0, ((0, 8),)),
        "state_taps": bell_draw(splits[5], (CONV_WIDTH, GROUP_COUNT * 2 * STATE_DIM), CONV_WIDTH ** -0.5, 3.0, ((1, 8),)),
        "state_bias": bell_draw(splits[6], (GROUP_COUNT * 2 * STATE_DIM,), 0.5, 3.0, ((0, 8),)),
        "step_raw": draw_step_raw(jax.random.fold_in(splits[14], 71), 0),
        "step_bias": jnp.clip(jax.random.uniform(splits[8], (HEAD_COUNT,), jnp.float32, -0.5, 0.5) * level_of(splits[8], (HEAD_COUNT,), ((0, 8),), -0.4, 0.0), -0.5, 0.5),
        "decay_log": draw_decay_log(jax.random.fold_in(splits[14], 71), 0),
        "skip_gain": jnp.clip(0.5 + 1.0 * jax.random.uniform(splits[10], (HEAD_COUNT,), jnp.float32) ** level_of(splits[10], (HEAD_COUNT,), ((0, 8),), -0.2, 0.2), 0.5, 1.5),
        "norm_gain": jnp.clip(1.0 + 0.1 * jax.random.normal(splits[11], (INNER_DIM,), jnp.float32), 0.5, 1.5).astype(jnp.bfloat16),
        "out_weight": noise_with(splits[12], (INNER_DIM, OUT_WIDTH), INNER_DIM ** -0.5, 0.09375, ((0, 8), (1, 32)), (0, 1, 32, 2.75)),
        "sequence_lengths": uneven(splits[13], SEQ_COUNT, PACKED_TOKENS, PACKED_TOKENS // 2, 2).astype(jnp.int32),
    }


HIGHEST = lax.Precision.HIGHEST
EPSILON = 1e-05

def segment_of(positions, sequence_lengths):
    starts = jnp.cumsum(sequence_lengths) - sequence_lengths
    hits = (positions[:, None] >= starts[None, :]).astype(jnp.int32)
    return lax.optimization_barrier(jnp.sum(hits, axis=1)) - 1

def causal_conv(extended, seg_extended, tap_table, bias_row):
    tap_count = tap_table.shape[0]
    length = extended.shape[0] - tap_count + 1
    current = seg_extended[tap_count - 1:]
    summed = jnp.zeros((length, bias_row.shape[0]), jnp.float32) + bias_row.astype(jnp.float32)
    for start_shift in range(tap_count):
        kept_mask = (seg_extended[start_shift:start_shift + length] == current).astype(jnp.float32)
        summed = summed + tap_table[start_shift].astype(jnp.float32) * extended[start_shift:start_shift + length].astype(jnp.float32) * kept_mask[:, None]
    return jax.nn.silu(summed).astype(jnp.bfloat16)

def block_step(decay_rates, skip_gains, carried, inputs):
    state_now, seg_before = carried
    input_block, write_block, read_block, step_block, seg_block = inputs
    block_rows = input_block.shape[0]
    log_decay = -decay_rates[..., None] * step_block
    running = jnp.cumsum(log_decay, axis=2)
    input_vals = input_block.astype(jnp.float32)
    write_vecs = write_block.astype(jnp.float32)
    read_vecs = read_block.astype(jnp.float32)
    scores = jnp.einsum('ign,jgn->gij', read_vecs, write_vecs, precision=HIGHEST)
    row_index = lax.broadcasted_iota(jnp.int32, (block_rows, block_rows), 0)
    col_index = lax.broadcasted_iota(jnp.int32, (block_rows, block_rows), 1)
    linked = (row_index >= col_index) & (seg_block[:, None] == seg_block[None, :])
    spread = running[..., :, None] - running[..., None, :]
    decays = jnp.where(linked, jnp.exp(jnp.where(linked, spread, 0.0)), 0.0)
    scaled = input_vals * jnp.transpose(step_block, (2, 0, 1))[..., None]
    within = jnp.einsum('ghij,jghp->ighp', decays * scores[:, None], scaled, precision=HIGHEST)
    alive_mask = (seg_block == seg_before).astype(jnp.float32)
    entering = jnp.transpose(alive_mask * jnp.exp(running), (2, 0, 1))
    carried_out = jnp.einsum('ign,ghpn->ighp', read_vecs, state_now, precision=HIGHEST) * entering[..., None]
    outputs = within + carried_out + skip_gains[..., None] * input_vals
    last_seg = seg_block[block_rows - 1]
    closing = (seg_block == last_seg).astype(jnp.float32) * jnp.exp(running[..., block_rows - 1:] - running)
    weighted = scaled * jnp.transpose(closing, (2, 0, 1))[..., None]
    kept = (alive_mask[block_rows - 1] * jnp.exp(running[..., block_rows - 1]))[..., None, None]
    new_state = kept * state_now + jnp.einsum('jghp,jgn->ghpn', weighted, write_vecs, precision=HIGHEST)
    return ((new_state, last_seg), outputs)

def reference(inner_input, state_input, gate_input, inner_taps, inner_bias, state_taps, state_bias, step_raw, step_bias, decay_log, skip_gain, norm_gain, out_weight, sequence_lengths):
    positions = lax.iota(jnp.int32, PACKED_TOKENS + CONV_WIDTH - 1) - (CONV_WIDTH - 1)
    seg_extended = segment_of(positions, sequence_lengths)
    seg_local = seg_extended[CONV_WIDTH - 1:]
    group_width = INNER_DIM // GROUP_COUNT
    group_heads = HEAD_COUNT // GROUP_COUNT
    pair_width = 2 * STATE_DIM
    block_count = PACKED_TOKENS // BLOCK_LEN

    def one_group(items):
        inner_part, state_part, gate_part, inner_tap, inner_off, state_tap, state_off, raw_part, bias_part, log_part, residual_skip_term, gain_part = items
        pad_inner = jnp.zeros((CONV_WIDTH - 1, group_width), jnp.bfloat16)
        inner_conv = causal_conv(jnp.concatenate([pad_inner, inner_part]), seg_extended, inner_tap, inner_off)
        pad_state = jnp.zeros((CONV_WIDTH - 1, pair_width), jnp.bfloat16)
        state_conv = causal_conv(jnp.concatenate([pad_state, state_part]), seg_extended, state_tap, state_off)
        vectors = state_conv.reshape(PACKED_TOKENS, 1, 2, STATE_DIM)
        steps_all = jax.nn.softplus(raw_part + bias_part[:, None]).reshape(1, group_heads, PACKED_TOKENS)
        decay_rates = jnp.exp(log_part).reshape(1, group_heads)
        sequence = (inner_conv.reshape(block_count, BLOCK_LEN, 1, group_heads, HEAD_DIM), vectors[:, :, 0].reshape(block_count, BLOCK_LEN, 1, STATE_DIM), vectors[:, :, 1].reshape(block_count, BLOCK_LEN, 1, STATE_DIM), jnp.transpose(steps_all.reshape(1, group_heads, block_count, BLOCK_LEN), (2, 0, 1, 3)), seg_local.reshape(block_count, BLOCK_LEN))
        start_carry = (jnp.zeros((1, group_heads, HEAD_DIM, STATE_DIM), jnp.float32), seg_extended[CONV_WIDTH - 2])
        stepper = partial(block_step, decay_rates, residual_skip_term.reshape(1, group_heads))
        _, outputs = lax.scan(stepper, start_carry, sequence)
        y_all = outputs.reshape(PACKED_TOKENS, group_width)
        gated = y_all * jax.nn.silu(gate_part.astype(jnp.float32))
        mean_sq = lax.optimization_barrier(jnp.mean(gated * gated, axis=1, keepdims=True))
        return (gated * lax.rsqrt(mean_sq + EPSILON) * gain_part.astype(jnp.float32)).astype(jnp.bfloat16)
    items = (jnp.transpose(inner_input.reshape(PACKED_TOKENS, GROUP_COUNT, group_width), (1, 0, 2)), jnp.transpose(state_input.reshape(PACKED_TOKENS, GROUP_COUNT, pair_width), (1, 0, 2)), jnp.transpose(gate_input.reshape(PACKED_TOKENS, GROUP_COUNT, group_width), (1, 0, 2)), jnp.transpose(inner_taps.reshape(CONV_WIDTH, GROUP_COUNT, group_width), (1, 0, 2)), inner_bias.reshape(GROUP_COUNT, group_width), jnp.transpose(state_taps.reshape(CONV_WIDTH, GROUP_COUNT, pair_width), (1, 0, 2)), state_bias.reshape(GROUP_COUNT, pair_width), step_raw.reshape(GROUP_COUNT, group_heads, PACKED_TOKENS), step_bias.reshape(GROUP_COUNT, group_heads), decay_log.reshape(GROUP_COUNT, group_heads), skip_gain.reshape(GROUP_COUNT, group_heads), norm_gain.reshape(GROUP_COUNT, group_width))
    normed_groups = lax.map(one_group, items)
    per_block = GROUP_COUNT // N_HEAD
    normed_sets = normed_groups.reshape(N_HEAD, per_block, PACKED_TOKENS, group_width)
    weight_sets = out_weight.reshape(N_HEAD, per_block, group_width, OUT_WIDTH)

    def add_block(total_sum, pair):
        normed_set, weight_set = pair
        partial_sum = jnp.zeros((PACKED_TOKENS, OUT_WIDTH), jnp.float32)
        for member in range(per_block):
            partial_sum = partial_sum + jnp.dot(normed_set[member], weight_set[member], preferred_element_type=jnp.float32)
        rounded = lax.optimization_barrier(partial_sum.astype(jnp.bfloat16))
        return (total_sum + rounded.astype(jnp.float32), None)
    total_sum, _ = lax.scan(add_block, jnp.zeros((PACKED_TOKENS, OUT_WIDTH), jnp.float32), (normed_sets, weight_sets))
    return total_sum.astype(jnp.bfloat16)
```

```python
import jax
import jax.numpy as jnp
import numpy as np
from jax import lax
from jax.sharding import Mesh
from jax.sharding import PartitionSpec as P

HEAD_DIM = 64
STATE_DIM = 256
BLOCK_LEN = 256


HIGHEST = lax.Precision.HIGHEST
EPSILON = 1e-05
SEQ = ("sx", "sz")


def segment_of(positions, sequence_lengths):
    starts = jnp.cumsum(sequence_lengths) - sequence_lengths
    hits = (positions[:, None] >= starts[None, :]).astype(jnp.int32)
    return jnp.sum(hits, axis=1) - 1


def causal_conv(extended, seg_extended, tap_table, bias_row):
    tap_count = tap_table.shape[0]
    length = extended.shape[0] - tap_count + 1
    current = seg_extended[tap_count - 1 :]
    summed = jnp.zeros((length, bias_row.shape[0]), jnp.float32) + bias_row.astype(jnp.float32)
    for start_shift in range(tap_count):
        kept_mask = (seg_extended[start_shift : start_shift + length] == current).astype(
            jnp.float32
        )
        summed = (
            summed
            + tap_table[start_shift].astype(jnp.float32)
            * extended[start_shift : start_shift + length].astype(jnp.float32)
            * kept_mask[:, None]
        )
    return jax.nn.silu(summed).astype(jnp.bfloat16)


def exclusive_weights(factors, place):
    n = factors.shape[0]
    idx = jnp.arange(n)
    j = idx[:, None]
    t = idx[None, :]
    between = (t > j) & (t < place)
    prods = jnp.prod(jnp.where(between[:, :, None], factors[None, :, :], 1.0), axis=1)
    return jnp.where((idx < place)[:, None], prods, 0.0)


def pack_state(state, factor):
    heads = factor.shape[0]
    flat = state.reshape(-1, state.shape[-1])
    extra = jnp.zeros((8, flat.shape[1]), jnp.float32).at[0, :heads].set(factor)
    return jnp.concatenate([flat, extra], axis=0).astype(jnp.bfloat16)


def unpack_state(gathered, heads):
    rows = gathered.shape[1] - 8
    states = gathered[:, :rows].astype(jnp.float32).reshape(
        gathered.shape[0], heads, rows // heads, gathered.shape[2]
    )
    factors = gathered[:, rows, :heads].astype(jnp.float32)
    return states, factors


def combine(states, factors, place):
    weights = exclusive_weights(factors, place)
    return jnp.sum(weights[:, :, None, None] * states, axis=0)


def per_device(
    inner_input,
    state_input,
    gate_input,
    inner_taps,
    inner_bias,
    state_taps,
    state_bias,
    step_raw,
    step_bias,
    decay_log,
    skip_gain,
    norm_gain,
    out_weight,
    sequence_lengths,
):
    tok_rows = inner_input.shape[0]
    inner_width = inner_input.shape[1]
    heads = step_raw.shape[0]
    groups = state_input.shape[1] // (2 * STATE_DIM)
    per_group = heads // groups
    tap_count = inner_taps.shape[0]
    chunks = tok_rows // BLOCK_LEN
    L = BLOCK_LEN
    nz = lax.axis_size("sz")
    nseq = lax.axis_size("sx") * nz
    place = lax.axis_index("sx") * nz + lax.axis_index("sz")
    first_row = place * tok_rows

    half = out_weight.shape[0] // 2
    weight_a = lax.all_gather(out_weight[:half], SEQ, axis=1, tiled=True)

    positions = first_row + lax.iota(jnp.int32, tok_rows + tap_count - 1) - (tap_count - 1)
    seg_extended = segment_of(positions, sequence_lengths)
    seg_local = seg_extended[tap_count - 1 :]
    seg_before = seg_extended[tap_count - 2]
    tail_rows = jnp.concatenate(
        [inner_input[tok_rows - tap_count + 1 :], state_input[tok_rows - tap_count + 1 :]], axis=1
    )
    received = lax.ppermute(tail_rows, SEQ, [(s, s + 1) for s in range(nseq - 1)])
    inner_conv = causal_conv(
        jnp.concatenate([received[:, :inner_width], inner_input]),
        seg_extended,
        inner_taps,
        inner_bias,
    )
    state_conv = causal_conv(
        jnp.concatenate([received[:, inner_width:], state_input]),
        seg_extended,
        state_taps,
        state_bias,
    )
    u = inner_conv.reshape(chunks, L, groups, per_group, HEAD_DIM)
    vectors = state_conv.reshape(chunks, L, groups, 2, STATE_DIM)
    write_b = vectors[:, :, :, 0]
    read_c = vectors[:, :, :, 1]
    steps = jax.nn.softplus(step_raw + step_bias[:, None]).reshape(
        groups, per_group, chunks, L
    )
    rates = jnp.exp(decay_log).reshape(groups, per_group)
    gains = skip_gain.reshape(groups, per_group)
    running = jnp.cumsum(-rates[..., None, None] * steps, axis=3)
    seg_c = seg_local.reshape(chunks, L)
    seg_prev = jnp.concatenate([seg_before[None], seg_c[:-1, L - 1]])
    alive = (seg_c == seg_prev[:, None]).astype(jnp.float32)
    last = running[..., L - 1 :]

    u32 = u.astype(jnp.float32)
    scaled = u32 * jnp.transpose(steps, (2, 3, 0, 1))[..., None]

    closing = (seg_c == seg_c[:, L - 1 :]).astype(jnp.float32) * jnp.exp(last - running)
    weighted = scaled * jnp.transpose(closing, (2, 3, 0, 1))[..., None]
    chunk_states = jnp.einsum(
        "cjghp,cjgn->cghpn", weighted, write_b.astype(jnp.float32), precision=HIGHEST
    )
    kept = alive[:, L - 1] * jnp.exp(last[..., 0])
    kept = jnp.transpose(kept, (2, 0, 1))
    shard_state = chunk_states[0]
    shard_factor = kept[0]
    for c in range(1, chunks):
        shard_state = kept[c][..., None, None] * shard_state + chunk_states[c]
        shard_factor = shard_factor * kept[c]

    row = lax.all_gather(pack_state(shard_state, shard_factor.reshape(-1)), "sz")
    row_states, row_factors = unpack_state(row, heads)
    zpos = lax.axis_index("sz")
    in_row = combine(row_states, row_factors, zpos)
    row_decay = jnp.prod(jnp.where((jnp.arange(nz) < zpos)[:, None], row_factors, 1.0), axis=0)
    row_total = combine(row_states, row_factors, nz)
    row_total_factor = jnp.prod(row_factors, axis=0)
    rows = lax.all_gather(pack_state(row_total, row_total_factor), "sx")
    rows_states, rows_factors = unpack_state(rows, heads)
    before_rows = combine(rows_states, rows_factors, lax.axis_index("sx"))
    state_in = (row_decay[:, None, None] * before_rows + in_row).reshape(
        groups, per_group, HEAD_DIM, STATE_DIM
    )

    weight_b_src, rows = lax.optimization_barrier((out_weight[half:], rows))
    weight_b = lax.all_gather(weight_b_src, SEQ, axis=1, tiled=True)

    read32 = read_c.astype(jnp.float32)
    scores = jnp.einsum(
        "cign,cjgn->gcij", read_c, write_b, preferred_element_type=jnp.float32
    )
    row_index = lax.broadcasted_iota(jnp.int32, (L, L), 0)
    col_index = lax.broadcasted_iota(jnp.int32, (L, L), 1)
    linked = (row_index >= col_index)[None] & (seg_c[:, :, None] == seg_c[:, None, :])
    spread = running[..., :, None] - running[..., None, :]
    decays = jnp.where(linked, jnp.exp(jnp.where(linked, spread, 0.0)), 0.0)
    within = jnp.einsum(
        "ghcij,cjghp->cighp", decays * scores[:, None], scaled, precision=HIGHEST
    )

    entering = [state_in]
    for c in range(1, chunks):
        entering.append(kept[c - 1][..., None, None] * entering[-1] + chunk_states[c - 1])
    entering = jnp.stack(entering)
    carried = jnp.einsum("cign,cghpn->cighp", read32, entering, precision=HIGHEST)
    enter_scale = jnp.transpose(alive[None, None] * jnp.exp(running), (2, 3, 0, 1))
    outputs = within + carried * enter_scale[..., None] + gains[..., None] * u32

    y_all = outputs.reshape(tok_rows, groups, per_group * HEAD_DIM)
    gated = y_all * jax.nn.silu(gate_input.astype(jnp.float32)).reshape(
        tok_rows, groups, per_group * HEAD_DIM
    )
    mean_sq = jnp.mean(gated * gated, axis=2, keepdims=True)
    gain_rows = norm_gain.astype(jnp.float32).reshape(groups, per_group * HEAD_DIM)
    normed = (
        (gated * lax.rsqrt(mean_sq + EPSILON) * gain_rows)
        .astype(jnp.bfloat16)
        .reshape(tok_rows, inner_width)
    )
    partial_out = jnp.dot(
        normed[:, :half], weight_a, preferred_element_type=jnp.float32
    ) + jnp.dot(normed[:, half:], weight_b, preferred_element_type=jnp.float32)
    return lax.psum_scatter(
        partial_out.astype(jnp.bfloat16), "head", scatter_dimension=1, tiled=True
    )


def split_seq(mesh):
    seq_devices = mesh.devices[:, 0]
    try:
        nx = len({d.coords[0] for d in seq_devices})
    except AttributeError:
        nx = 1
    nseq = seq_devices.shape[0]
    return Mesh(
        mesh.devices.reshape(nx, nseq // nx, mesh.devices.shape[1]), ("sx", "sz", "head")
    )


def solution(mesh):
    inner = split_seq(mesh)
    in_specs = (
        P(SEQ, "head"),
        P(SEQ, "head"),
        P(SEQ, "head"),
        P(None, "head"),
        P("head"),
        P(None, "head"),
        P("head"),
        P("head", SEQ),
        P("head"),
        P("head"),
        P("head"),
        P("head"),
        P("head", SEQ),
        P(),
    )
    out_specs = P(SEQ, "head")
    return jax.shard_map(
        per_device, mesh=inner, in_specs=in_specs, out_specs=out_specs, check_vma=False
    )
```

```python
import jax
import jax.numpy as jnp
import numpy as np
from jax import lax
from jax.sharding import Mesh
from jax.sharding import PartitionSpec as P

HEAD_DIM = 64
STATE_DIM = 256
BLOCK_LEN = 256


HIGHEST = lax.Precision.HIGHEST
EPSILON = 1e-05
SEQ = ("sx", "sz")


def segment_of(positions, sequence_lengths):
    starts = jnp.cumsum(sequence_lengths) - sequence_lengths
    hits = (positions[:, None] >= starts[None, :]).astype(jnp.int32)
    return jnp.sum(hits, axis=1) - 1


def causal_conv(extended, seg_extended, tap_table, bias_row):
    tap_count = tap_table.shape[0]
    length = extended.shape[0] - tap_count + 1
    current = seg_extended[tap_count - 1 :]
    summed = jnp.zeros((length, bias_row.shape[0]), jnp.float32) + bias_row.astype(jnp.float32)
    for start_shift in range(tap_count):
        kept_mask = (seg_extended[start_shift : start_shift + length] == current).astype(
            jnp.float32
        )
        summed = (
            summed
            + tap_table[start_shift].astype(jnp.float32)
            * extended[start_shift : start_shift + length].astype(jnp.float32)
            * kept_mask[:, None]
        )
    return jax.nn.silu(summed).astype(jnp.bfloat16)


def exclusive_weights(factors, place):
    n = factors.shape[0]
    idx = jnp.arange(n)
    j = idx[:, None]
    t = idx[None, :]
    between = (t > j) & (t < place)
    prods = jnp.prod(jnp.where(between[:, :, None], factors[None, :, :], 1.0), axis=1)
    return jnp.where((idx < place)[:, None], prods, 0.0)


def pack_state(state, factor):
    heads = factor.shape[0]
    flat = state.reshape(-1, state.shape[-1])
    extra = jnp.zeros((8, flat.shape[1]), jnp.float32).at[0, :heads].set(factor)
    return jnp.concatenate([flat, extra], axis=0).astype(jnp.bfloat16)


def unpack_state(gathered, heads):
    rows = gathered.shape[1] - 8
    states = gathered[:, :rows].astype(jnp.float32).reshape(
        gathered.shape[0], heads, rows // heads, gathered.shape[2]
    )
    factors = gathered[:, rows, :heads].astype(jnp.float32)
    return states, factors


def combine(states, factors, place):
    weights = exclusive_weights(factors, place)
    return jnp.sum(weights[:, :, None, None] * states, axis=0)


def per_device(
    inner_input,
    state_input,
    gate_input,
    inner_taps,
    inner_bias,
    state_taps,
    state_bias,
    step_raw,
    step_bias,
    decay_log,
    skip_gain,
    norm_gain,
    out_weight,
    sequence_lengths,
):
    tok_rows = inner_input.shape[0]
    inner_width = inner_input.shape[1]
    heads = step_raw.shape[0]
    groups = state_input.shape[1] // (2 * STATE_DIM)
    per_group = heads // groups
    tap_count = inner_taps.shape[0]
    chunks = tok_rows // BLOCK_LEN
    L = BLOCK_LEN
    nz = lax.axis_size("sz")
    nseq = lax.axis_size("sx") * nz
    place = lax.axis_index("sx") * nz + lax.axis_index("sz")
    first_row = place * tok_rows

    weights = lax.all_gather(out_weight, SEQ, axis=1, tiled=True)

    positions = first_row + lax.iota(jnp.int32, tok_rows + tap_count - 1) - (tap_count - 1)
    seg_extended = segment_of(positions, sequence_lengths)
    seg_local = seg_extended[tap_count - 1 :]
    seg_before = seg_extended[tap_count - 2]
    tail_rows = jnp.concatenate(
        [inner_input[tok_rows - tap_count + 1 :], state_input[tok_rows - tap_count + 1 :]], axis=1
    )
    received = lax.ppermute(tail_rows, SEQ, [(s, s + 1) for s in range(nseq - 1)])
    inner_conv = causal_conv(
        jnp.concatenate([received[:, :inner_width], inner_input]),
        seg_extended,
        inner_taps,
        inner_bias,
    )
    state_conv = causal_conv(
        jnp.concatenate([received[:, inner_width:], state_input]),
        seg_extended,
        state_taps,
        state_bias,
    )
    u = inner_conv.reshape(chunks, L, groups, per_group, HEAD_DIM)
    vectors = state_conv.reshape(chunks, L, groups, 2, STATE_DIM)
    write_b = vectors[:, :, :, 0]
    read_c = vectors[:, :, :, 1]
    steps = jax.nn.softplus(step_raw + step_bias[:, None]).reshape(
        groups, per_group, chunks, L
    )
    rates = jnp.exp(decay_log).reshape(groups, per_group)
    gains = skip_gain.reshape(groups, per_group)
    running = jnp.cumsum(-rates[..., None, None] * steps, axis=3)
    seg_c = seg_local.reshape(chunks, L)
    seg_prev = jnp.concatenate([seg_before[None], seg_c[:-1, L - 1]])
    alive = (seg_c == seg_prev[:, None]).astype(jnp.float32)
    last = running[..., L - 1 :]

    u32 = u.astype(jnp.float32)
    scaled = u32 * jnp.transpose(steps, (2, 3, 0, 1))[..., None]

    closing = (seg_c == seg_c[:, L - 1 :]).astype(jnp.float32) * jnp.exp(last - running)
    weighted = scaled * jnp.transpose(closing, (2, 3, 0, 1))[..., None]
    chunk_states = jnp.einsum(
        "cjghp,cjgn->cghpn", weighted, write_b.astype(jnp.float32), precision=HIGHEST
    )
    kept = alive[:, L - 1] * jnp.exp(last[..., 0])
    kept = jnp.transpose(kept, (2, 0, 1))
    shard_state = chunk_states[0]
    shard_factor = kept[0]
    for c in range(1, chunks):
        shard_state = kept[c][..., None, None] * shard_state + chunk_states[c]
        shard_factor = shard_factor * kept[c]

    packed, weights = lax.optimization_barrier(
        (pack_state(shard_state, shard_factor.reshape(-1)), weights)
    )
    row = lax.all_gather(packed, "sz")
    row_states, row_factors = unpack_state(row, heads)
    zpos = lax.axis_index("sz")
    in_row = combine(row_states, row_factors, zpos)
    row_decay = jnp.prod(jnp.where((jnp.arange(nz) < zpos)[:, None], row_factors, 1.0), axis=0)
    row_total = combine(row_states, row_factors, nz)
    row_total_factor = jnp.prod(row_factors, axis=0)
    rows = lax.all_gather(pack_state(row_total, row_total_factor), "sx")
    rows_states, rows_factors = unpack_state(rows, heads)
    before_rows = combine(rows_states, rows_factors, lax.axis_index("sx"))
    state_in = (row_decay[:, None, None] * before_rows + in_row).reshape(
        groups, per_group, HEAD_DIM, STATE_DIM
    )

    read32 = read_c.astype(jnp.float32)
    scores = jnp.einsum(
        "cign,cjgn->gcij", read_c, write_b, preferred_element_type=jnp.float32
    )
    row_index = lax.broadcasted_iota(jnp.int32, (L, L), 0)
    col_index = lax.broadcasted_iota(jnp.int32, (L, L), 1)
    linked = (row_index >= col_index)[None] & (seg_c[:, :, None] == seg_c[:, None, :])
    spread = running[..., :, None] - running[..., None, :]
    decays = jnp.where(linked, jnp.exp(jnp.where(linked, spread, 0.0)), 0.0)
    within = jnp.einsum(
        "ghcij,cjghp->cighp", decays * scores[:, None], scaled, precision=HIGHEST
    )

    entering = [state_in]
    for c in range(1, chunks):
        entering.append(kept[c - 1][..., None, None] * entering[-1] + chunk_states[c - 1])
    entering = jnp.stack(entering)
    carried = jnp.einsum("cign,cghpn->cighp", read32, entering, precision=HIGHEST)
    enter_scale = jnp.transpose(alive[None, None] * jnp.exp(running), (2, 3, 0, 1))
    outputs = within + carried * enter_scale[..., None] + gains[..., None] * u32

    y_all = outputs.reshape(tok_rows, groups, per_group * HEAD_DIM)
    gated = y_all * jax.nn.silu(gate_input.astype(jnp.float32)).reshape(
        tok_rows, groups, per_group * HEAD_DIM
    )
    mean_sq = jnp.mean(gated * gated, axis=2, keepdims=True)
    gain_rows = norm_gain.astype(jnp.float32).reshape(groups, per_group * HEAD_DIM)
    normed = (
        (gated * lax.rsqrt(mean_sq + EPSILON) * gain_rows)
        .astype(jnp.bfloat16)
        .reshape(tok_rows, inner_width)
    )
    partial_out = jnp.dot(normed, weights, preferred_element_type=jnp.float32)
    return lax.psum_scatter(
        partial_out.astype(jnp.bfloat16), "head", scatter_dimension=1, tiled=True
    )


def split_seq(mesh):
    seq_devices = mesh.devices[:, 0]
    try:
        nx = len({d.coords[0] for d in seq_devices})
    except AttributeError:
        nx = 1
    nseq = seq_devices.shape[0]
    return Mesh(
        mesh.devices.reshape(nx, nseq // nx, mesh.devices.shape[1]), ("sx", "sz", "head")
    )


def solution(mesh):
    inner = split_seq(mesh)
    in_specs = (
        P(SEQ, "head"),
        P(SEQ, "head"),
        P(SEQ, "head"),
        P(None, "head"),
        P("head"),
        P(None, "head"),
        P("head"),
        P("head", SEQ),
        P("head"),
        P("head"),
        P("head"),
        P("head"),
        P("head", SEQ),
        P(),
    )
    out_specs = P(SEQ, "head")
    return jax.shard_map(
        per_device, mesh=inner, in_specs=in_specs, out_specs=out_specs, check_vma=False
    )
```

```python
import jax
import jax.numpy as jnp
import numpy as np
from jax import lax
from jax.sharding import Mesh
from jax.sharding import PartitionSpec as P

HEAD_DIM = 64
STATE_DIM = 256
BLOCK_LEN = 256


HIGHEST = lax.Precision.HIGHEST
EPSILON = 1e-05
SEQ = ("sx", "sz")


def segment_of(positions, sequence_lengths):
    starts = jnp.cumsum(sequence_lengths) - sequence_lengths
    hits = (positions[:, None] >= starts[None, :]).astype(jnp.int32)
    return jnp.sum(hits, axis=1) - 1


def causal_conv(extended, seg_extended, tap_table, bias_row):
    tap_count = tap_table.shape[0]
    length = extended.shape[0] - tap_count + 1
    current = seg_extended[tap_count - 1 :]
    summed = jnp.zeros((length, bias_row.shape[0]), jnp.float32) + bias_row.astype(jnp.float32)
    for start_shift in range(tap_count):
        kept_mask = (seg_extended[start_shift : start_shift + length] == current).astype(
            jnp.float32
        )
        summed = (
            summed
            + tap_table[start_shift].astype(jnp.float32)
            * extended[start_shift : start_shift + length].astype(jnp.float32)
            * kept_mask[:, None]
        )
    return jax.nn.silu(summed).astype(jnp.bfloat16)


def exclusive_weights(factors, place):
    n = factors.shape[0]
    idx = jnp.arange(n)
    j = idx[:, None]
    t = idx[None, :]
    between = (t > j) & (t < place)
    prods = jnp.prod(jnp.where(between[:, :, None], factors[None, :, :], 1.0), axis=1)
    return jnp.where((idx < place)[:, None], prods, 0.0)


def pack_state(state, factor):
    heads = factor.shape[0]
    flat = state.reshape(-1, state.shape[-1])
    extra = jnp.zeros((8, flat.shape[1]), jnp.float32).at[0, :heads].set(factor)
    return jnp.concatenate([flat, extra], axis=0).astype(jnp.bfloat16)


def unpack_state(gathered, heads):
    rows = gathered.shape[1] - 8
    states = gathered[:, :rows].astype(jnp.float32).reshape(
        gathered.shape[0], heads, rows // heads, gathered.shape[2]
    )
    factors = gathered[:, rows, :heads].astype(jnp.float32)
    return states, factors


def gather_rows(packed, axis):
    count = lax.axis_size(axis)
    return lax.all_to_all(
        jnp.broadcast_to(packed[None], (count,) + packed.shape), axis, 0, 0, tiled=False
    )


def combine(states, factors, place):
    weights = exclusive_weights(factors, place)
    return jnp.sum(weights[:, :, None, None] * states, axis=0)


def per_device(
    inner_input,
    state_input,
    gate_input,
    inner_taps,
    inner_bias,
    state_taps,
    state_bias,
    step_raw,
    step_bias,
    decay_log,
    skip_gain,
    norm_gain,
    out_weight,
    sequence_lengths,
):
    tok_rows = inner_input.shape[0]
    inner_width = inner_input.shape[1]
    heads = step_raw.shape[0]
    groups = state_input.shape[1] // (2 * STATE_DIM)
    per_group = heads // groups
    tap_count = inner_taps.shape[0]
    chunks = tok_rows // BLOCK_LEN
    L = BLOCK_LEN
    nz = lax.axis_size("sz")
    nseq = lax.axis_size("sx") * nz
    place = lax.axis_index("sx") * nz + lax.axis_index("sz")
    first_row = place * tok_rows

    weights = lax.all_gather(out_weight, SEQ, axis=1, tiled=True)

    positions = first_row + lax.iota(jnp.int32, tok_rows + tap_count - 1) - (tap_count - 1)
    seg_extended = segment_of(positions, sequence_lengths)
    seg_local = seg_extended[tap_count - 1 :]
    seg_before = seg_extended[tap_count - 2]
    tail_rows = jnp.concatenate(
        [inner_input[tok_rows - tap_count + 1 :], state_input[tok_rows - tap_count + 1 :]], axis=1
    )
    received = lax.ppermute(tail_rows, SEQ, [(s, s + 1) for s in range(nseq - 1)])
    inner_conv = causal_conv(
        jnp.concatenate([received[:, :inner_width], inner_input]),
        seg_extended,
        inner_taps,
        inner_bias,
    )
    state_conv = causal_conv(
        jnp.concatenate([received[:, inner_width:], state_input]),
        seg_extended,
        state_taps,
        state_bias,
    )
    u = inner_conv.reshape(chunks, L, groups, per_group, HEAD_DIM)
    vectors = state_conv.reshape(chunks, L, groups, 2, STATE_DIM)
    write_b = vectors[:, :, :, 0]
    read_c = vectors[:, :, :, 1]
    steps = jax.nn.softplus(step_raw + step_bias[:, None]).reshape(
        groups, per_group, chunks, L
    )
    rates = jnp.exp(decay_log).reshape(groups, per_group)
    gains = skip_gain.reshape(groups, per_group)
    running = jnp.cumsum(-rates[..., None, None] * steps, axis=3)
    seg_c = seg_local.reshape(chunks, L)
    seg_prev = jnp.concatenate([seg_before[None], seg_c[:-1, L - 1]])
    alive = (seg_c == seg_prev[:, None]).astype(jnp.float32)
    last = running[..., L - 1 :]

    u32 = u.astype(jnp.float32)
    scaled = u32 * jnp.transpose(steps, (2, 3, 0, 1))[..., None]

    closing = (seg_c == seg_c[:, L - 1 :]).astype(jnp.float32) * jnp.exp(last - running)
    weighted = scaled * jnp.transpose(closing, (2, 3, 0, 1))[..., None]
    chunk_states = jnp.einsum(
        "cjghp,cjgn->cghpn", weighted, write_b.astype(jnp.float32), precision=HIGHEST
    )
    kept = alive[:, L - 1] * jnp.exp(last[..., 0])
    kept = jnp.transpose(kept, (2, 0, 1))
    shard_state = chunk_states[0]
    shard_factor = kept[0]
    for c in range(1, chunks):
        shard_state = kept[c][..., None, None] * shard_state + chunk_states[c]
        shard_factor = shard_factor * kept[c]

    row = gather_rows(pack_state(shard_state, shard_factor.reshape(-1)), "sz")
    row_states, row_factors = unpack_state(row, heads)
    zpos = lax.axis_index("sz")
    in_row = combine(row_states, row_factors, zpos)
    row_decay = jnp.prod(jnp.where((jnp.arange(nz) < zpos)[:, None], row_factors, 1.0), axis=0)
    row_total = combine(row_states, row_factors, nz)
    row_total_factor = jnp.prod(row_factors, axis=0)
    rows = gather_rows(pack_state(row_total, row_total_factor), "sx")
    rows_states, rows_factors = unpack_state(rows, heads)
    before_rows = combine(rows_states, rows_factors, lax.axis_index("sx"))
    state_in = (row_decay[:, None, None] * before_rows + in_row).reshape(
        groups, per_group, HEAD_DIM, STATE_DIM
    )

    read32 = read_c.astype(jnp.float32)
    scores = jnp.einsum(
        "cign,cjgn->gcij", read_c, write_b, preferred_element_type=jnp.float32
    )
    row_index = lax.broadcasted_iota(jnp.int32, (L, L), 0)
    col_index = lax.broadcasted_iota(jnp.int32, (L, L), 1)
    linked = (row_index >= col_index)[None] & (seg_c[:, :, None] == seg_c[:, None, :])
    spread = running[..., :, None] - running[..., None, :]
    decays = jnp.where(linked, jnp.exp(jnp.where(linked, spread, 0.0)), 0.0)
    within = jnp.einsum(
        "ghcij,cjghp->cighp", decays * scores[:, None], scaled, precision=HIGHEST
    )

    entering = [state_in]
    for c in range(1, chunks):
        entering.append(kept[c - 1][..., None, None] * entering[-1] + chunk_states[c - 1])
    entering = jnp.stack(entering)
    carried = jnp.einsum("cign,cghpn->cighp", read32, entering, precision=HIGHEST)
    enter_scale = jnp.transpose(alive[None, None] * jnp.exp(running), (2, 3, 0, 1))
    outputs = within + carried * enter_scale[..., None] + gains[..., None] * u32

    y_all = outputs.reshape(tok_rows, groups, per_group * HEAD_DIM)
    gated = y_all * jax.nn.silu(gate_input.astype(jnp.float32)).reshape(
        tok_rows, groups, per_group * HEAD_DIM
    )
    mean_sq = jnp.mean(gated * gated, axis=2, keepdims=True)
    gain_rows = norm_gain.astype(jnp.float32).reshape(groups, per_group * HEAD_DIM)
    normed = (
        (gated * lax.rsqrt(mean_sq + EPSILON) * gain_rows)
        .astype(jnp.bfloat16)
        .reshape(tok_rows, inner_width)
    )
    partial_out = jnp.dot(normed, weights, preferred_element_type=jnp.float32)
    return lax.psum_scatter(
        partial_out.astype(jnp.bfloat16), "head", scatter_dimension=1, tiled=True
    )


def split_seq(mesh):
    seq_devices = mesh.devices[:, 0]
    try:
        nx = len({d.coords[0] for d in seq_devices})
    except AttributeError:
        nx = 1
    nseq = seq_devices.shape[0]
    return Mesh(
        mesh.devices.reshape(nx, nseq // nx, mesh.devices.shape[1]), ("sx", "sz", "head")
    )


def solution(mesh):
    inner = split_seq(mesh)
    in_specs = (
        P(SEQ, "head"),
        P(SEQ, "head"),
        P(SEQ, "head"),
        P(None, "head"),
        P("head"),
        P(None, "head"),
        P("head"),
        P("head", SEQ),
        P("head"),
        P("head"),
        P("head"),
        P("head"),
        P("head", SEQ),
        P(),
    )
    out_specs = P(SEQ, "head")
    return jax.shard_map(
        per_device, mesh=inner, in_specs=in_specs, out_specs=out_specs, check_vma=False
    )
```

```python
import jax
import jax.numpy as jnp
import numpy as np
from jax import lax
from jax.sharding import Mesh
from jax.sharding import PartitionSpec as P

HEAD_DIM = 64
STATE_DIM = 256
BLOCK_LEN = 256


HIGHEST = lax.Precision.HIGHEST
EPSILON = 1e-05
SEQ = ("sx", "sz")


def segment_of(positions, sequence_lengths):
    starts = jnp.cumsum(sequence_lengths) - sequence_lengths
    hits = (positions[:, None] >= starts[None, :]).astype(jnp.int32)
    return jnp.sum(hits, axis=1) - 1


def causal_conv(extended, seg_extended, tap_table, bias_row):
    tap_count = tap_table.shape[0]
    length = extended.shape[0] - tap_count + 1
    current = seg_extended[tap_count - 1 :]
    summed = jnp.zeros((length, bias_row.shape[0]), jnp.float32) + bias_row.astype(jnp.float32)
    for start_shift in range(tap_count):
        kept_mask = (seg_extended[start_shift : start_shift + length] == current).astype(
            jnp.float32
        )
        summed = (
            summed
            + tap_table[start_shift].astype(jnp.float32)
            * extended[start_shift : start_shift + length].astype(jnp.float32)
            * kept_mask[:, None]
        )
    return jax.nn.silu(summed).astype(jnp.bfloat16)


def exclusive_weights(factors, place):
    n = factors.shape[0]
    idx = jnp.arange(n)
    j = idx[:, None]
    t = idx[None, :]
    between = (t > j) & (t < place)
    prods = jnp.prod(jnp.where(between[:, :, None], factors[None, :, :], 1.0), axis=1)
    return jnp.where((idx < place)[:, None], prods, 0.0)


def pack_state(state, factor):
    heads = factor.shape[0]
    flat = state.reshape(-1, state.shape[-1])
    extra = jnp.zeros((8, flat.shape[1]), jnp.float32).at[0, :heads].set(factor)
    return jnp.concatenate([flat, extra], axis=0).astype(jnp.bfloat16)


def unpack_state(gathered, heads):
    rows = gathered.shape[1] - 8
    states = gathered[:, :rows].astype(jnp.float32).reshape(
        gathered.shape[0], heads, rows // heads, gathered.shape[2]
    )
    factors = gathered[:, rows, :heads].astype(jnp.float32)
    return states, factors


def gather_rows(packed, axis):
    count = lax.axis_size(axis)
    return lax.all_to_all(
        jnp.broadcast_to(packed[None], (count,) + packed.shape), axis, 0, 0, tiled=False
    )


def combine(states, factors, place):
    weights = exclusive_weights(factors, place)
    return jnp.sum(weights[:, :, None, None] * states, axis=0)


def per_device(
    inner_input,
    state_input,
    gate_input,
    inner_taps,
    inner_bias,
    state_taps,
    state_bias,
    step_raw,
    step_bias,
    decay_log,
    skip_gain,
    norm_gain,
    out_weight,
    sequence_lengths,
):
    tok_rows = inner_input.shape[0]
    inner_width = inner_input.shape[1]
    heads = step_raw.shape[0]
    groups = state_input.shape[1] // (2 * STATE_DIM)
    per_group = heads // groups
    tap_count = inner_taps.shape[0]
    chunks = tok_rows // BLOCK_LEN
    L = BLOCK_LEN
    nz = lax.axis_size("sz")
    nseq = lax.axis_size("sx") * nz
    place = lax.axis_index("sx") * nz + lax.axis_index("sz")
    first_row = place * tok_rows

    weights_z = lax.all_gather(out_weight, "sz", axis=1, tiled=True)

    positions = first_row + lax.iota(jnp.int32, tok_rows + tap_count - 1) - (tap_count - 1)
    seg_extended = segment_of(positions, sequence_lengths)
    seg_local = seg_extended[tap_count - 1 :]
    seg_before = seg_extended[tap_count - 2]
    tail_rows = jnp.concatenate(
        [inner_input[tok_rows - tap_count + 1 :], state_input[tok_rows - tap_count + 1 :]], axis=1
    )
    received = lax.ppermute(tail_rows, SEQ, [(s, s + 1) for s in range(nseq - 1)])
    inner_conv = causal_conv(
        jnp.concatenate([received[:, :inner_width], inner_input]),
        seg_extended,
        inner_taps,
        inner_bias,
    )
    state_conv = causal_conv(
        jnp.concatenate([received[:, inner_width:], state_input]),
        seg_extended,
        state_taps,
        state_bias,
    )
    u = inner_conv.reshape(chunks, L, groups, per_group, HEAD_DIM)
    vectors = state_conv.reshape(chunks, L, groups, 2, STATE_DIM)
    write_b = vectors[:, :, :, 0]
    read_c = vectors[:, :, :, 1]
    steps = jax.nn.softplus(step_raw + step_bias[:, None]).reshape(
        groups, per_group, chunks, L
    )
    rates = jnp.exp(decay_log).reshape(groups, per_group)
    gains = skip_gain.reshape(groups, per_group)
    running = jnp.cumsum(-rates[..., None, None] * steps, axis=3)
    seg_c = seg_local.reshape(chunks, L)
    seg_prev = jnp.concatenate([seg_before[None], seg_c[:-1, L - 1]])
    alive = (seg_c == seg_prev[:, None]).astype(jnp.float32)
    last = running[..., L - 1 :]

    u32 = u.astype(jnp.float32)
    scaled = u32 * jnp.transpose(steps, (2, 3, 0, 1))[..., None]

    closing = (seg_c == seg_c[:, L - 1 :]).astype(jnp.float32) * jnp.exp(last - running)
    weighted = scaled * jnp.transpose(closing, (2, 3, 0, 1))[..., None]
    chunk_states = jnp.einsum(
        "cjghp,cjgn->cghpn", weighted, write_b.astype(jnp.float32), precision=HIGHEST
    )
    kept = alive[:, L - 1] * jnp.exp(last[..., 0])
    kept = jnp.transpose(kept, (2, 0, 1))
    shard_state = chunk_states[0]
    shard_factor = kept[0]
    for c in range(1, chunks):
        shard_state = kept[c][..., None, None] * shard_state + chunk_states[c]
        shard_factor = shard_factor * kept[c]

    packed, weights_z = lax.optimization_barrier(
        (pack_state(shard_state, shard_factor.reshape(-1)), weights_z)
    )
    weights = lax.all_gather(weights_z, "sx", axis=1, tiled=True)
    row = gather_rows(packed, "sz")
    row_states, row_factors = unpack_state(row, heads)
    zpos = lax.axis_index("sz")
    in_row = combine(row_states, row_factors, zpos)
    row_decay = jnp.prod(jnp.where((jnp.arange(nz) < zpos)[:, None], row_factors, 1.0), axis=0)
    row_total = combine(row_states, row_factors, nz)
    row_total_factor = jnp.prod(row_factors, axis=0)
    row_pack, weights = lax.optimization_barrier(
        (pack_state(row_total, row_total_factor), weights)
    )
    rows = lax.all_gather(row_pack, "sx")
    rows_states, rows_factors = unpack_state(rows, heads)
    before_rows = combine(rows_states, rows_factors, lax.axis_index("sx"))
    state_in = (row_decay[:, None, None] * before_rows + in_row).reshape(
        groups, per_group, HEAD_DIM, STATE_DIM
    )

    read32 = read_c.astype(jnp.float32)
    scores = jnp.einsum(
        "cign,cjgn->gcij", read_c, write_b, preferred_element_type=jnp.float32
    )
    row_index = lax.broadcasted_iota(jnp.int32, (L, L), 0)
    col_index = lax.broadcasted_iota(jnp.int32, (L, L), 1)
    linked = (row_index >= col_index)[None] & (seg_c[:, :, None] == seg_c[:, None, :])
    spread = running[..., :, None] - running[..., None, :]
    decays = jnp.where(linked, jnp.exp(jnp.where(linked, spread, 0.0)), 0.0)
    within = jnp.einsum(
        "ghcij,cjghp->cighp", decays * scores[:, None], scaled, precision=HIGHEST
    )

    entering = [state_in]
    for c in range(1, chunks):
        entering.append(kept[c - 1][..., None, None] * entering[-1] + chunk_states[c - 1])
    entering = jnp.stack(entering)
    carried = jnp.einsum("cign,cghpn->cighp", read32, entering, precision=HIGHEST)
    enter_scale = jnp.transpose(alive[None, None] * jnp.exp(running), (2, 3, 0, 1))
    outputs = within + carried * enter_scale[..., None] + gains[..., None] * u32

    y_all = outputs.reshape(tok_rows, groups, per_group * HEAD_DIM)
    gated = y_all * jax.nn.silu(gate_input.astype(jnp.float32)).reshape(
        tok_rows, groups, per_group * HEAD_DIM
    )
    mean_sq = jnp.mean(gated * gated, axis=2, keepdims=True)
    gain_rows = norm_gain.astype(jnp.float32).reshape(groups, per_group * HEAD_DIM)
    normed = (
        (gated * lax.rsqrt(mean_sq + EPSILON) * gain_rows)
        .astype(jnp.bfloat16)
        .reshape(tok_rows, inner_width)
    )
    partial_out = jnp.dot(normed, weights, preferred_element_type=jnp.float32)
    return lax.psum_scatter(
        partial_out.astype(jnp.bfloat16), "head", scatter_dimension=1, tiled=True
    )


def split_seq(mesh):
    seq_devices = mesh.devices[:, 0]
    try:
        nx = len({d.coords[0] for d in seq_devices})
    except AttributeError:
        nx = 1
    nseq = seq_devices.shape[0]
    return Mesh(
        mesh.devices.reshape(nx, nseq // nx, mesh.devices.shape[1]), ("sx", "sz", "head")
    )


def solution(mesh):
    inner = split_seq(mesh)
    in_specs = (
        P(SEQ, "head"),
        P(SEQ, "head"),
        P(SEQ, "head"),
        P(None, "head"),
        P("head"),
        P(None, "head"),
        P("head"),
        P("head", SEQ),
        P("head"),
        P("head"),
        P("head"),
        P("head"),
        P("head", SEQ),
        P(),
    )
    out_specs = P(SEQ, "head")
    return jax.shard_map(
        per_device, mesh=inner, in_specs=in_specs, out_specs=out_specs, check_vma=False
    )
```

```python
import jax
import jax.numpy as jnp
import numpy as np
from jax import lax
from jax.sharding import Mesh
from jax.sharding import PartitionSpec as P

HEAD_DIM = 64
STATE_DIM = 256
BLOCK_LEN = 256


HIGHEST = lax.Precision.HIGHEST
EPSILON = 1e-05
SEQ = ("sx", "sz1", "sz2")
LEVELS = ("sz2", "sz1", "sx")


def segment_of(positions, sequence_lengths):
    starts = jnp.cumsum(sequence_lengths) - sequence_lengths
    hits = (positions[:, None] >= starts[None, :]).astype(jnp.int32)
    return jnp.sum(hits, axis=1) - 1


def causal_conv(extended, seg_extended, tap_table, bias_row):
    tap_count = tap_table.shape[0]
    length = extended.shape[0] - tap_count + 1
    current = seg_extended[tap_count - 1 :]
    summed = jnp.zeros((length, bias_row.shape[0]), jnp.float32) + bias_row.astype(jnp.float32)
    for start_shift in range(tap_count):
        kept_mask = (seg_extended[start_shift : start_shift + length] == current).astype(
            jnp.float32
        )
        summed = (
            summed
            + tap_table[start_shift].astype(jnp.float32)
            * extended[start_shift : start_shift + length].astype(jnp.float32)
            * kept_mask[:, None]
        )
    return jax.nn.silu(summed).astype(jnp.bfloat16)


def exclusive_weights(factors, place):
    n = factors.shape[0]
    idx = jnp.arange(n)
    j = idx[:, None]
    t = idx[None, :]
    between = (t > j) & (t < place)
    prods = jnp.prod(jnp.where(between[:, :, None], factors[None, :, :], 1.0), axis=1)
    return jnp.where((idx < place)[:, None], prods, 0.0)


def pack_state(state, factor):
    heads = factor.shape[0]
    flat = state.reshape(-1, state.shape[-1])
    extra = jnp.zeros((8, flat.shape[1]), jnp.float32).at[0, :heads].set(factor)
    return jnp.concatenate([flat, extra], axis=0).astype(jnp.bfloat16)


def unpack_state(gathered, heads):
    rows = gathered.shape[1] - 8
    states = gathered[:, :rows].astype(jnp.float32).reshape(
        gathered.shape[0], heads, rows // heads, gathered.shape[2]
    )
    factors = gathered[:, rows, :heads].astype(jnp.float32)
    return states, factors


def combine(states, factors, place):
    weights = exclusive_weights(factors, place)
    return jnp.sum(weights[:, :, None, None] * states, axis=0)


def per_device(
    inner_input,
    state_input,
    gate_input,
    inner_taps,
    inner_bias,
    state_taps,
    state_bias,
    step_raw,
    step_bias,
    decay_log,
    skip_gain,
    norm_gain,
    out_weight,
    sequence_lengths,
):
    tok_rows = inner_input.shape[0]
    inner_width = inner_input.shape[1]
    heads = step_raw.shape[0]
    groups = state_input.shape[1] // (2 * STATE_DIM)
    per_group = heads // groups
    tap_count = inner_taps.shape[0]
    chunks = tok_rows // BLOCK_LEN
    L = BLOCK_LEN
    nseq = 1
    place = 0
    for name in SEQ:
        nseq = nseq * lax.axis_size(name)
        place = place * lax.axis_size(name) + lax.axis_index(name)
    first_row = place * tok_rows

    weights = lax.all_gather(out_weight, SEQ, axis=1, tiled=True)

    positions = first_row + lax.iota(jnp.int32, tok_rows + tap_count - 1) - (tap_count - 1)
    seg_extended = segment_of(positions, sequence_lengths)
    seg_local = seg_extended[tap_count - 1 :]
    seg_before = seg_extended[tap_count - 2]
    tail_rows = jnp.concatenate(
        [inner_input[tok_rows - tap_count + 1 :], state_input[tok_rows - tap_count + 1 :]], axis=1
    )
    received = lax.ppermute(tail_rows, SEQ, [(s, s + 1) for s in range(nseq - 1)])
    inner_conv = causal_conv(
        jnp.concatenate([received[:, :inner_width], inner_input]),
        seg_extended,
        inner_taps,
        inner_bias,
    )
    state_conv = causal_conv(
        jnp.concatenate([received[:, inner_width:], state_input]),
        seg_extended,
        state_taps,
        state_bias,
    )
    u = inner_conv.reshape(chunks, L, groups, per_group, HEAD_DIM)
    vectors = state_conv.reshape(chunks, L, groups, 2, STATE_DIM)
    write_b = vectors[:, :, :, 0]
    read_c = vectors[:, :, :, 1]
    steps = jax.nn.softplus(step_raw + step_bias[:, None]).reshape(
        groups, per_group, chunks, L
    )
    rates = jnp.exp(decay_log).reshape(groups, per_group)
    gains = skip_gain.reshape(groups, per_group)
    running = jnp.cumsum(-rates[..., None, None] * steps, axis=3)
    seg_c = seg_local.reshape(chunks, L)
    seg_prev = jnp.concatenate([seg_before[None], seg_c[:-1, L - 1]])
    alive = (seg_c == seg_prev[:, None]).astype(jnp.float32)
    last = running[..., L - 1 :]

    u32 = u.astype(jnp.float32)
    scaled = u32 * jnp.transpose(steps, (2, 3, 0, 1))[..., None]

    closing = (seg_c == seg_c[:, L - 1 :]).astype(jnp.float32) * jnp.exp(last - running)
    weighted = scaled * jnp.transpose(closing, (2, 3, 0, 1))[..., None]
    chunk_states = jnp.einsum(
        "cjghp,cjgn->cghpn", weighted, write_b.astype(jnp.float32), precision=HIGHEST
    )
    kept = alive[:, L - 1] * jnp.exp(last[..., 0])
    kept = jnp.transpose(kept, (2, 0, 1))
    shard_state = chunk_states[0]
    shard_factor = kept[0]
    for c in range(1, chunks):
        shard_state = kept[c][..., None, None] * shard_state + chunk_states[c]
        shard_factor = shard_factor * kept[c]

    packed, weights = lax.optimization_barrier(
        (pack_state(shard_state, shard_factor.reshape(-1)), weights)
    )
    state_in = jnp.zeros_like(shard_state)
    scale = jnp.ones_like(shard_factor)
    for level, name in enumerate(LEVELS):
        gathered = lax.all_gather(packed, name)
        member_states, member_factors = unpack_state(gathered, heads)
        pos = lax.axis_index(name)
        count = lax.axis_size(name)
        state_in = state_in + scale[..., None, None] * combine(
            member_states, member_factors, pos
        )
        scale = scale * jnp.prod(
            jnp.where((jnp.arange(count) < pos)[:, None], member_factors, 1.0), axis=0
        )
        if level + 1 < len(LEVELS):
            packed = pack_state(
                combine(member_states, member_factors, count),
                jnp.prod(member_factors, axis=0),
            )
    state_in = state_in.reshape(groups, per_group, HEAD_DIM, STATE_DIM)

    read32 = read_c.astype(jnp.float32)
    scores = jnp.einsum(
        "cign,cjgn->gcij", read_c, write_b, preferred_element_type=jnp.float32
    )
    row_index = lax.broadcasted_iota(jnp.int32, (L, L), 0)
    col_index = lax.broadcasted_iota(jnp.int32, (L, L), 1)
    linked = (row_index >= col_index)[None] & (seg_c[:, :, None] == seg_c[:, None, :])
    spread = running[..., :, None] - running[..., None, :]
    decays = jnp.where(linked, jnp.exp(jnp.where(linked, spread, 0.0)), 0.0)
    within = jnp.einsum(
        "ghcij,cjghp->cighp", decays * scores[:, None], scaled, precision=HIGHEST
    )

    entering = [state_in]
    for c in range(1, chunks):
        entering.append(kept[c - 1][..., None, None] * entering[-1] + chunk_states[c - 1])
    entering = jnp.stack(entering)
    carried = jnp.einsum("cign,cghpn->cighp", read32, entering, precision=HIGHEST)
    enter_scale = jnp.transpose(alive[None, None] * jnp.exp(running), (2, 3, 0, 1))
    outputs = within + carried * enter_scale[..., None] + gains[..., None] * u32

    y_all = outputs.reshape(tok_rows, groups, per_group * HEAD_DIM)
    gated = y_all * jax.nn.silu(gate_input.astype(jnp.float32)).reshape(
        tok_rows, groups, per_group * HEAD_DIM
    )
    mean_sq = jnp.mean(gated * gated, axis=2, keepdims=True)
    gain_rows = norm_gain.astype(jnp.float32).reshape(groups, per_group * HEAD_DIM)
    normed = (
        (gated * lax.rsqrt(mean_sq + EPSILON) * gain_rows)
        .astype(jnp.bfloat16)
        .reshape(tok_rows, inner_width)
    )
    partial_out = jnp.dot(normed, weights, preferred_element_type=jnp.float32)
    return lax.psum_scatter(
        partial_out.astype(jnp.bfloat16), "head", scatter_dimension=1, tiled=True
    )


def split_seq(mesh):
    seq_devices = mesh.devices[:, 0]
    try:
        nx = len({d.coords[0] for d in seq_devices})
    except AttributeError:
        nx = 1
    nseq = seq_devices.shape[0]
    nz = nseq // nx
    fine = 4 if nz % 4 == 0 else nz
    return Mesh(
        mesh.devices.reshape(nx, nz // fine, fine, mesh.devices.shape[1]),
        ("sx", "sz1", "sz2", "head"),
    )


def solution(mesh):
    inner = split_seq(mesh)
    in_specs = (
        P(SEQ, "head"),
        P(SEQ, "head"),
        P(SEQ, "head"),
        P(None, "head"),
        P("head"),
        P(None, "head"),
        P("head"),
        P("head", SEQ),
        P("head"),
        P("head"),
        P("head"),
        P("head"),
        P("head", SEQ),
        P(),
    )
    out_specs = P(SEQ, "head")
    return jax.shard_map(
        per_device, mesh=inner, in_specs=in_specs, out_specs=out_specs, check_vma=False
    )
```

```python
import jax
import jax.numpy as jnp
import numpy as np
from jax import lax
from jax.sharding import Mesh
from jax.sharding import PartitionSpec as P

HEAD_DIM = 64
STATE_DIM = 256
BLOCK_LEN = 256


HIGHEST = lax.Precision.HIGHEST
EPSILON = 1e-05
SEQ = ("sx", "sz")


def segment_of(positions, sequence_lengths):
    starts = jnp.cumsum(sequence_lengths) - sequence_lengths
    hits = (positions[:, None] >= starts[None, :]).astype(jnp.int32)
    return jnp.sum(hits, axis=1) - 1


def causal_conv(extended, seg_extended, tap_table, bias_row):
    tap_count = tap_table.shape[0]
    length = extended.shape[0] - tap_count + 1
    current = seg_extended[tap_count - 1 :]
    summed = jnp.zeros((length, bias_row.shape[0]), jnp.float32) + bias_row.astype(jnp.float32)
    for start_shift in range(tap_count):
        kept_mask = (seg_extended[start_shift : start_shift + length] == current).astype(
            jnp.float32
        )
        summed = (
            summed
            + tap_table[start_shift].astype(jnp.float32)
            * extended[start_shift : start_shift + length].astype(jnp.float32)
            * kept_mask[:, None]
        )
    return jax.nn.silu(summed).astype(jnp.bfloat16)


def exclusive_weights(factors, place):
    n = factors.shape[0]
    idx = jnp.arange(n)
    j = idx[:, None]
    t = idx[None, :]
    between = (t > j) & (t < place)
    prods = jnp.prod(jnp.where(between[:, :, None], factors[None, :, :], 1.0), axis=1)
    return jnp.where((idx < place)[:, None], prods, 0.0)


def pack_state(state, factor):
    heads = factor.shape[0]
    flat = state.reshape(-1, state.shape[-1])
    extra = jnp.zeros((8, flat.shape[1]), jnp.float32).at[0, :heads].set(factor)
    return jnp.concatenate([flat, extra], axis=0).astype(jnp.bfloat16)


def unpack_state(gathered, heads):
    rows = gathered.shape[1] - 8
    states = gathered[:, :rows].astype(jnp.float32).reshape(
        gathered.shape[0], heads, rows // heads, gathered.shape[2]
    )
    factors = gathered[:, rows, :heads].astype(jnp.float32)
    return states, factors


def combine(states, factors, place):
    weights = exclusive_weights(factors, place)
    return jnp.sum(weights[:, :, None, None] * states, axis=0)


def per_device(
    inner_input,
    state_input,
    gate_input,
    inner_taps,
    inner_bias,
    state_taps,
    state_bias,
    step_raw,
    step_bias,
    decay_log,
    skip_gain,
    norm_gain,
    out_weight,
    sequence_lengths,
):
    tok_rows = inner_input.shape[0]
    inner_width = inner_input.shape[1]
    heads = step_raw.shape[0]
    groups = state_input.shape[1] // (2 * STATE_DIM)
    per_group = heads // groups
    tap_count = inner_taps.shape[0]
    chunks = tok_rows // BLOCK_LEN
    L = BLOCK_LEN
    nz = lax.axis_size("sz")
    nseq = lax.axis_size("sx") * nz
    place = lax.axis_index("sx") * nz + lax.axis_index("sz")
    first_row = place * tok_rows

    weights = lax.all_gather(out_weight, SEQ, axis=1, tiled=True)

    positions = first_row + lax.iota(jnp.int32, tok_rows + tap_count - 1) - (tap_count - 1)
    seg_extended = segment_of(positions, sequence_lengths)
    seg_local = seg_extended[tap_count - 1 :]
    seg_before = seg_extended[tap_count - 2]
    tail_rows = jnp.concatenate(
        [inner_input[tok_rows - tap_count + 1 :], state_input[tok_rows - tap_count + 1 :]], axis=1
    )
    received = lax.ppermute(tail_rows, SEQ, [(s, s + 1) for s in range(nseq - 1)])
    inner_conv = causal_conv(
        jnp.concatenate([received[:, :inner_width], inner_input]),
        seg_extended,
        inner_taps,
        inner_bias,
    )
    state_conv = causal_conv(
        jnp.concatenate([received[:, inner_width:], state_input]),
        seg_extended,
        state_taps,
        state_bias,
    )
    u = inner_conv.reshape(chunks, L, groups, per_group, HEAD_DIM)
    vectors = state_conv.reshape(chunks, L, groups, 2, STATE_DIM)
    write_b = vectors[:, :, :, 0]
    read_c = vectors[:, :, :, 1]
    steps = jax.nn.softplus(step_raw + step_bias[:, None]).reshape(
        groups, per_group, chunks, L
    )
    rates = jnp.exp(decay_log).reshape(groups, per_group)
    gains = skip_gain.reshape(groups, per_group)
    running = jnp.cumsum(-rates[..., None, None] * steps, axis=3)
    seg_c = seg_local.reshape(chunks, L)
    seg_prev = jnp.concatenate([seg_before[None], seg_c[:-1, L - 1]])
    alive = (seg_c == seg_prev[:, None]).astype(jnp.float32)
    last = running[..., L - 1 :]

    u32 = u.astype(jnp.float32)
    scaled = u32 * jnp.transpose(steps, (2, 3, 0, 1))[..., None]

    closing = (seg_c == seg_c[:, L - 1 :]).astype(jnp.float32) * jnp.exp(last - running)
    weighted = scaled * jnp.transpose(closing, (2, 3, 0, 1))[..., None]
    chunk_states = jnp.einsum(
        "cjghp,cjgn->cghpn", weighted, write_b.astype(jnp.float32), precision=HIGHEST
    )
    kept = alive[:, L - 1] * jnp.exp(last[..., 0])
    kept = jnp.transpose(kept, (2, 0, 1))
    shard_state = chunk_states[0]
    shard_factor = kept[0]
    for c in range(1, chunks):
        shard_state = kept[c][..., None, None] * shard_state + chunk_states[c]
        shard_factor = shard_factor * kept[c]

    packed, weights = lax.optimization_barrier(
        (pack_state(shard_state, shard_factor.reshape(-1)), weights)
    )
    row = lax.all_gather(packed, "sz")
    row_states, row_factors = unpack_state(row, heads)
    zpos = lax.axis_index("sz")
    row_total = combine(row_states, row_factors, nz)
    row_total_factor = jnp.prod(row_factors, axis=0)
    row_pack = pack_state(row_total, row_total_factor)
    row_states, row_factors, row_pack = lax.optimization_barrier(
        (row_states, row_factors, row_pack)
    )
    rows = lax.all_gather(row_pack, "sx")
    in_row = combine(row_states, row_factors, zpos)
    row_decay = jnp.prod(jnp.where((jnp.arange(nz) < zpos)[:, None], row_factors, 1.0), axis=0)
    rows_states, rows_factors = unpack_state(rows, heads)
    before_rows = combine(rows_states, rows_factors, lax.axis_index("sx"))
    state_in = (row_decay[:, None, None] * before_rows + in_row).reshape(
        groups, per_group, HEAD_DIM, STATE_DIM
    )

    read32 = read_c.astype(jnp.float32)
    scores = jnp.einsum(
        "cign,cjgn->gcij", read_c, write_b, preferred_element_type=jnp.float32
    )
    row_index = lax.broadcasted_iota(jnp.int32, (L, L), 0)
    col_index = lax.broadcasted_iota(jnp.int32, (L, L), 1)
    linked = (row_index >= col_index)[None] & (seg_c[:, :, None] == seg_c[:, None, :])
    spread = running[..., :, None] - running[..., None, :]
    decays = jnp.where(linked, jnp.exp(jnp.where(linked, spread, 0.0)), 0.0)
    within = jnp.einsum(
        "ghcij,cjghp->cighp", decays * scores[:, None], scaled, precision=HIGHEST
    )

    entering = [state_in]
    for c in range(1, chunks):
        entering.append(kept[c - 1][..., None, None] * entering[-1] + chunk_states[c - 1])
    entering = jnp.stack(entering)
    carried = jnp.einsum("cign,cghpn->cighp", read32, entering, precision=HIGHEST)
    enter_scale = jnp.transpose(alive[None, None] * jnp.exp(running), (2, 3, 0, 1))
    outputs = within + carried * enter_scale[..., None] + gains[..., None] * u32

    y_all = outputs.reshape(tok_rows, groups, per_group * HEAD_DIM)
    gated = y_all * jax.nn.silu(gate_input.astype(jnp.float32)).reshape(
        tok_rows, groups, per_group * HEAD_DIM
    )
    mean_sq = jnp.mean(gated * gated, axis=2, keepdims=True)
    gain_rows = norm_gain.astype(jnp.float32).reshape(groups, per_group * HEAD_DIM)
    normed = (
        (gated * lax.rsqrt(mean_sq + EPSILON) * gain_rows)
        .astype(jnp.bfloat16)
        .reshape(tok_rows, inner_width)
    )
    partial_out = jnp.dot(normed, weights, preferred_element_type=jnp.float32)
    return lax.psum_scatter(
        partial_out.astype(jnp.bfloat16), "head", scatter_dimension=1, tiled=True
    )


def split_seq(mesh):
    seq_devices = mesh.devices[:, 0]
    try:
        nx = len({d.coords[0] for d in seq_devices})
    except AttributeError:
        nx = 1
    nseq = seq_devices.shape[0]
    return Mesh(
        mesh.devices.reshape(nx, nseq // nx, mesh.devices.shape[1]), ("sx", "sz", "head")
    )


def solution(mesh):
    inner = split_seq(mesh)
    in_specs = (
        P(SEQ, "head"),
        P(SEQ, "head"),
        P(SEQ, "head"),
        P(None, "head"),
        P("head"),
        P(None, "head"),
        P("head"),
        P("head", SEQ),
        P("head"),
        P("head"),
        P("head"),
        P("head"),
        P("head", SEQ),
        P(),
    )
    out_specs = P(SEQ, "head")
    return jax.shard_map(
        per_device, mesh=inner, in_specs=in_specs, out_specs=out_specs, check_vma=False
    )
```

```python
import jax
import jax.numpy as jnp
import numpy as np
from jax import lax
from jax.sharding import Mesh
from jax.sharding import PartitionSpec as P

HEAD_DIM = 64
STATE_DIM = 256
BLOCK_LEN = 256


HIGHEST = lax.Precision.HIGHEST
EPSILON = 1e-05
SEQ = ("sx", "sz")


def segment_of(positions, sequence_lengths):
    starts = jnp.cumsum(sequence_lengths) - sequence_lengths
    hits = (positions[:, None] >= starts[None, :]).astype(jnp.int32)
    return jnp.sum(hits, axis=1) - 1


def causal_conv(extended, seg_extended, tap_table, bias_row):
    tap_count = tap_table.shape[0]
    length = extended.shape[0] - tap_count + 1
    current = seg_extended[tap_count - 1 :]
    summed = jnp.zeros((length, bias_row.shape[0]), jnp.float32) + bias_row.astype(jnp.float32)
    for start_shift in range(tap_count):
        kept_mask = (seg_extended[start_shift : start_shift + length] == current).astype(
            jnp.float32
        )
        summed = (
            summed
            + tap_table[start_shift].astype(jnp.float32)
            * extended[start_shift : start_shift + length].astype(jnp.float32)
            * kept_mask[:, None]
        )
    return jax.nn.silu(summed).astype(jnp.bfloat16)


def exclusive_weights(factors, place):
    n = factors.shape[0]
    idx = jnp.arange(n)
    j = idx[:, None]
    t = idx[None, :]
    between = (t > j) & (t < place)
    prods = jnp.prod(jnp.where(between[:, :, None], factors[None, :, :], 1.0), axis=1)
    return jnp.where((idx < place)[:, None], prods, 0.0)


def pack_state(state, factor):
    heads = factor.shape[0]
    flat = state.reshape(-1, state.shape[-1])
    extra = jnp.zeros((8, flat.shape[1]), jnp.float32).at[0, :heads].set(factor)
    return jnp.concatenate([flat, extra], axis=0).astype(jnp.bfloat16)


def unpack_state(gathered, heads):
    rows = gathered.shape[1] - 8
    states = gathered[:, :rows].astype(jnp.float32).reshape(
        gathered.shape[0], heads, rows // heads, gathered.shape[2]
    )
    factors = gathered[:, rows, :heads].astype(jnp.float32)
    return states, factors


def gather_rows(packed, axis):
    count = lax.axis_size(axis)
    return lax.all_to_all(
        jnp.broadcast_to(packed[None], (count,) + packed.shape), axis, 0, 0, tiled=False
    )


def combine(states, factors, place):
    weights = exclusive_weights(factors, place)
    return jnp.sum(weights[:, :, None, None] * states, axis=0)


def per_device(
    inner_input,
    state_input,
    gate_input,
    inner_taps,
    inner_bias,
    state_taps,
    state_bias,
    step_raw,
    step_bias,
    decay_log,
    skip_gain,
    norm_gain,
    out_weight,
    sequence_lengths,
):
    tok_rows = inner_input.shape[0]
    inner_width = inner_input.shape[1]
    heads = step_raw.shape[0]
    groups = state_input.shape[1] // (2 * STATE_DIM)
    per_group = heads // groups
    tap_count = inner_taps.shape[0]
    chunks = tok_rows // BLOCK_LEN
    L = BLOCK_LEN
    nz = lax.axis_size("sz")
    nseq = lax.axis_size("sx") * nz
    place = lax.axis_index("sx") * nz + lax.axis_index("sz")
    first_row = place * tok_rows

    weights = lax.all_gather(out_weight, SEQ, axis=1, tiled=True)

    positions = first_row + lax.iota(jnp.int32, tok_rows + tap_count - 1) - (tap_count - 1)
    seg_extended = segment_of(positions, sequence_lengths)
    seg_local = seg_extended[tap_count - 1 :]
    seg_before = seg_extended[tap_count - 2]
    tail_rows = jnp.concatenate(
        [inner_input[tok_rows - tap_count + 1 :], state_input[tok_rows - tap_count + 1 :]], axis=1
    )
    received = lax.ppermute(tail_rows, SEQ, [(s, s + 1) for s in range(nseq - 1)])
    inner_conv = causal_conv(
        jnp.concatenate([received[:, :inner_width], inner_input]),
        seg_extended,
        inner_taps,
        inner_bias,
    )
    state_conv = causal_conv(
        jnp.concatenate([received[:, inner_width:], state_input]),
        seg_extended,
        state_taps,
        state_bias,
    )
    u = inner_conv.reshape(chunks, L, groups, per_group, HEAD_DIM)
    vectors = state_conv.reshape(chunks, L, groups, 2, STATE_DIM)
    write_b = vectors[:, :, :, 0]
    read_c = vectors[:, :, :, 1]
    steps = jax.nn.softplus(step_raw + step_bias[:, None]).reshape(
        groups, per_group, chunks, L
    )
    rates = jnp.exp(decay_log).reshape(groups, per_group)
    gains = skip_gain.reshape(groups, per_group)
    running = jnp.cumsum(-rates[..., None, None] * steps, axis=3)
    seg_c = seg_local.reshape(chunks, L)
    seg_prev = jnp.concatenate([seg_before[None], seg_c[:-1, L - 1]])
    alive = (seg_c == seg_prev[:, None]).astype(jnp.float32)
    last = running[..., L - 1 :]

    u32 = u.astype(jnp.float32)
    scaled = u32 * jnp.transpose(steps, (2, 3, 0, 1))[..., None]

    closing = (seg_c == seg_c[:, L - 1 :]).astype(jnp.float32) * jnp.exp(last - running)
    weighted = scaled * jnp.transpose(closing, (2, 3, 0, 1))[..., None]
    chunk_states = jnp.einsum(
        "cjghp,cjgn->cghpn", weighted, write_b.astype(jnp.float32), precision=HIGHEST
    )
    kept = alive[:, L - 1] * jnp.exp(last[..., 0])
    kept = jnp.transpose(kept, (2, 0, 1))
    shard_state = chunk_states[0]
    shard_factor = kept[0]
    for c in range(1, chunks):
        shard_state = kept[c][..., None, None] * shard_state + chunk_states[c]
        shard_factor = shard_factor * kept[c]

    packed, weights = lax.optimization_barrier(
        (pack_state(shard_state, shard_factor.reshape(-1)), weights)
    )
    row = gather_rows(packed, "sz")
    row_states, row_factors = unpack_state(row, heads)
    zpos = lax.axis_index("sz")
    in_row = combine(row_states, row_factors, zpos)
    row_decay = jnp.prod(jnp.where((jnp.arange(nz) < zpos)[:, None], row_factors, 1.0), axis=0)
    row_total = combine(row_states, row_factors, nz)
    row_total_factor = jnp.prod(row_factors, axis=0)
    rows = gather_rows(pack_state(row_total, row_total_factor), "sx")
    rows_states, rows_factors = unpack_state(rows, heads)
    before_rows = combine(rows_states, rows_factors, lax.axis_index("sx"))
    state_in = (row_decay[:, None, None] * before_rows + in_row).reshape(
        groups, per_group, HEAD_DIM, STATE_DIM
    )

    read32 = read_c.astype(jnp.float32)
    scores = jnp.einsum(
        "cign,cjgn->gcij", read_c, write_b, preferred_element_type=jnp.float32
    )
    row_index = lax.broadcasted_iota(jnp.int32, (L, L), 0)
    col_index = lax.broadcasted_iota(jnp.int32, (L, L), 1)
    linked = (row_index >= col_index)[None] & (seg_c[:, :, None] == seg_c[:, None, :])
    spread = running[..., :, None] - running[..., None, :]
    decays = jnp.where(linked, jnp.exp(jnp.where(linked, spread, 0.0)), 0.0)
    within = jnp.einsum(
        "ghcij,cjghp->cighp", decays * scores[:, None], scaled, precision=HIGHEST
    )

    entering = [state_in]
    for c in range(1, chunks):
        entering.append(kept[c - 1][..., None, None] * entering[-1] + chunk_states[c - 1])
    entering = jnp.stack(entering)
    carried = jnp.einsum("cign,cghpn->cighp", read32, entering, precision=HIGHEST)
    enter_scale = jnp.transpose(alive[None, None] * jnp.exp(running), (2, 3, 0, 1))
    outputs = within + carried * enter_scale[..., None] + gains[..., None] * u32

    y_all = outputs.reshape(tok_rows, groups, per_group * HEAD_DIM)
    gated = y_all * jax.nn.silu(gate_input.astype(jnp.float32)).reshape(
        tok_rows, groups, per_group * HEAD_DIM
    )
    mean_sq = jnp.mean(gated * gated, axis=2, keepdims=True)
    gain_rows = norm_gain.astype(jnp.float32).reshape(groups, per_group * HEAD_DIM)
    normed = (
        (gated * lax.rsqrt(mean_sq + EPSILON) * gain_rows)
        .astype(jnp.bfloat16)
        .reshape(tok_rows, inner_width)
    )
    partial_out = jnp.dot(normed, weights, preferred_element_type=jnp.float32)
    return lax.psum_scatter(
        partial_out.astype(jnp.bfloat16), "head", scatter_dimension=1, tiled=True
    )


def split_seq(mesh):
    seq_devices = mesh.devices[:, 0]
    try:
        nx = len({d.coords[0] for d in seq_devices})
    except AttributeError:
        nx = 1
    nseq = seq_devices.shape[0]
    return Mesh(
        mesh.devices.reshape(nx, nseq // nx, mesh.devices.shape[1]), ("sx", "sz", "head")
    )


def solution(mesh):
    inner = split_seq(mesh)
    in_specs = (
        P(SEQ, "head"),
        P(SEQ, "head"),
        P(SEQ, "head"),
        P(None, "head"),
        P("head"),
        P(None, "head"),
        P("head"),
        P("head", SEQ),
        P("head"),
        P("head"),
        P("head"),
        P("head"),
        P("head", SEQ),
        P(),
    )
    out_specs = P(SEQ, "head")
    return jax.shard_map(
        per_device, mesh=inner, in_specs=in_specs, out_specs=out_specs, check_vma=False
    )
```
